32 devices in a mesh: tok: 16 (over z, x, core), head: 2 (over y).
Axes of the slice: x: 2, y: 2, z: 4, core: 2. Of those that a mesh axis runs over, the one named last changes fastest.
Arguments:
- inputs: bfloat16 [2, 8192, 2048], P(None, 'tok'), may hold values from -6 to 6
- projections: bfloat16 [3, 2048, 2048], P(None, None, 'head'), may hold values from -0.125 to 0.125
- lrate: float32 [2, 8192, 4], P(None, 'tok', 'head'), may hold values from 0.1 to 1
- fast_init: bfloat16 [4, 3, 384, 512], P('head'), may hold values from -0.25 to 0.25
- gain: float32 [2048], replicated, may hold values from 0.5 to 1.5
Outputs:
- normed: bfloat16 [2, 8192, 2048], P(None, ('tok', 'head'))
The draws below stay inside these ranges and needn't reach their ends.
All inputs are finite; a program needn't handle non-finite values.
Results may differ from the reference program's by a relative error of at most 0.018.
Values may be sent and summed in bfloat16 or wider, within the bound.
A program may use at most 128 MiB of HBM per device.

```python
import math
import jax
import jax.numpy as jnp
from jax import lax

D = 2048
HEADS = 4
HD = 512
F = 384
INNER = 2
GROUPS = 2
TOKENS = 8192


def block_scale(key, shape, cuts, low, largest):
    factor_of, own = 1.0, jax.random.fold_in(key, 6)
    for position, shards_of in cuts:
        heights = jnp.exp(jax.random.uniform(jax.random.fold_in(own, position), (shards_of,), jnp.float32, low / len(cuts), largest / len(cuts)))
        factor_of = factor_of * jnp.repeat(heights, shape[position] // shards_of).reshape([-1 if axis == position else 1 for axis in range(len(shape))])
    return factor_of


def bell_draw(stream_key, shape, spread, most, pieces=(), kind=jnp.bfloat16):
    loudness = block_scale(stream_key, shape, pieces, -0.22, 0.18) if pieces else 1.0
    drawn = jax.random.normal(stream_key, shape, jnp.float32) * spread * loudness
    return jnp.minimum(jnp.maximum(drawn, -most), most).astype(kind)


def setup_inputs(seed: int = 0) -> dict:
    arg_keys = jax.random.split(jax.random.key(seed), 6)
    inputs = bell_draw(arg_keys[0], (GROUPS, TOKENS, D), 1.0, 6.0, ((1, 16),))
    projections = bell_draw(arg_keys[1], (3, D, D), D ** -0.5, 0.125, ((2, 2),))
    lrate = jnp.clip(jnp.exp(math.log(1.0) - 2.3025851 * jax.random.uniform(arg_keys[2], (GROUPS, TOKENS, HEADS), jnp.float32) ** block_scale(arg_keys[2], (GROUPS, TOKENS, HEADS), ((1, 16), (2, 2)), -0.2, 0.2)), 0.1, 1.0)
    fast_init = bell_draw(arg_keys[3], (HEADS, 3, F, HD), HD ** -0.5, 0.25, ((0, 2),))
    gain = jnp.clip(1.0 + 0.1 * jax.random.normal(arg_keys[4], (D,), jnp.float32), 0.5, 1.5)
    return dict(inputs=inputs, projections=projections, lrate=lrate, fast_init=fast_init, gain=gain)


step_size = 4.0

def mult(form, left, right):
    return jnp.einsum(form, left.astype(jnp.float32), right.astype(jnp.float32))

def silu_parts(hidden):
    sigma = jax.nn.sigmoid(hidden)
    return (hidden * sigma, sigma * (1.0 + hidden * (1.0 - sigma)))

def token_gradients(weights, keys, values, rates):
    hidden = mult('htd,hfd->htf', keys, weights[:, 0])
    gated = mult('htd,hfd->htf', keys, weights[:, 1])
    act, slope = silu_parts(hidden)
    mixed = (act * gated).astype(jnp.bfloat16)
    signal = (-rates[:, :, None] * values.astype(jnp.float32)).astype(jnp.bfloat16)
    grad_second = mult('htf,htd->hfd', mixed, signal)
    back = mult('htd,hfd->htf', signal, weights[:, 2])
    grad_gate = (back * act).astype(jnp.bfloat16)
    grad_first = (back * gated * slope).astype(jnp.bfloat16)
    grad_one = mult('htf,htd->hfd', grad_first, keys)
    grad_three = mult('htf,htd->hfd', grad_gate, keys)
    return jnp.stack([grad_one, grad_three, grad_second], axis=1)

def refresh(weights, summed, target):
    frob = lax.optimization_barrier(jnp.sum(summed * summed, axis=(2, 3)))
    scale = step_size / jnp.sqrt(frob + 1e-06)
    update = weights.astype(jnp.float32) - scale[:, :, None, None] * summed
    length = jnp.sqrt(lax.optimization_barrier(jnp.sum(update * update, axis=-1, keepdims=True)) + 1e-06)
    return (update * (target / length)).astype(jnp.bfloat16)

def read_memory(weights, queries):
    hidden = mult('htd,hfd->htf', queries, weights[:, 0])
    gated = mult('htd,hfd->htf', queries, weights[:, 1])
    act, _ = silu_parts(hidden)
    mixed = (act * gated).astype(jnp.bfloat16)
    return mult('htf,hfd->htd', mixed, weights[:, 2]).astype(jnp.bfloat16)

def reference(inputs, projections, lrate, fast_init, gain):
    target = jnp.sqrt(lax.optimization_barrier(jnp.sum(jnp.square(fast_init.astype(jnp.float32)), axis=-1, keepdims=True)))
    weights = fast_init
    outputs = []
    for group in range(GROUPS):
        mapped = mult('td,sde->ste', inputs[group], projections).astype(jnp.bfloat16)
        split = mapped.reshape(3, TOKENS, HEADS, HD).transpose(0, 2, 1, 3)
        queries, keys, values = (split[0], split[1], split[2])
        rates = lrate[group].T
        for inner in range(INNER):
            summed = token_gradients(weights, keys, values, rates)
            weights = refresh(weights, summed, target)
        readout = read_memory(weights, queries)
        joined = readout.transpose(1, 0, 2).reshape(TOKENS, HEADS * HD).astype(jnp.float32)
        square_mean = lax.optimization_barrier(jnp.mean(joined * joined, axis=-1, keepdims=True))
        outputs.append((joined * lax.rsqrt(square_mean + 1e-06) * gain).astype(jnp.bfloat16))
    return jnp.stack(outputs)
```

```python
import functools

import jax
import jax.numpy as jnp
from jax import lax
from jax.experimental import pallas as pl
from jax.experimental.pallas import tpu as pltpu
from jax.sharding import PartitionSpec as P

INNER = 2
CORES = 2
STEP_SIZE = 4.0
EPS = 1e-06
MESH = pl.DeviceIdType.MESH
BLOCK = 16
NT = (((1,), (1,)), ((), ()))


def dot(left, right):
    return jnp.dot(left, right, preferred_element_type=jnp.float32)


def dot_nt(left, right):
    return lax.dot_general(left, right, NT, preferred_element_type=jnp.float32)


def train_kernel(
    tok_size, head_size, piece,
    own_ref, rec_ref, init_ref, gain_ref, out_ref,
    weights, target, hid, gat, bak, mixed, dgate, dfirst, rhid, rgat, rmix,
    gsend, rs_recv, whole, ro_send, ro_recv,
    rs_send_sem, rs_recv_sem, ag_send_sem, ag_recv_sem, ro_send_sem, ro_recv_sem,
):
    groups, tokens = own_ref.shape[1], own_ref.shape[2]
    hidden_units = init_ref.shape[1]
    peers = tok_size // CORES
    owners = hidden_units // piece
    quarter = tokens // head_size
    tok = lax.axis_index("tok")
    head = lax.axis_index("head")
    chip, core = tok // CORES, tok % CORES
    partner = chip * CORES + (1 - core)

    def peer(offset):
        return lax.rem(chip + offset, peers)

    def device_of(index):
        return {"tok": index * CORES + core, "head": head}

    def guarded(condition, work):
        if owners == peers:
            work()
        else:
            pl.when(condition)(work)

    exchanges = [(pos, off) for pos in range(CORES) for off in range(head_size) if (pos, off) != (0, 0)]

    def exchange_device(pos, off):
        return {"tok": tok if pos == 0 else partner, "head": lax.rem(head + off, head_size)}

    barrier = pltpu.get_barrier_semaphore()
    for off in range(1, peers):
        pl.semaphore_signal(barrier, inc=1, device_id=device_of(peer(off)), device_id_type=MESH)
    for pos, off in exchanges:
        pl.semaphore_signal(barrier, inc=1, device_id=exchange_device(pos, off), device_id_type=MESH)

    def rows(block):
        return pl.ds(pl.multiple_of(block * BLOCK, BLOCK), BLOCK)

    for m in range(3):
        def prepare(block, carry, m=m):
            start = init_ref[m, rows(block), :]
            weights[m, rows(block), :] = start
            start = start.astype(jnp.float32)
            target[m, rows(block), :] = jnp.sqrt(jnp.sum(start * start, axis=-1, keepdims=True))
            return carry

        lax.fori_loop(0, hidden_units // BLOCK, prepare, 0)

    pl.semaphore_wait(barrier, peers - 1 + len(exchanges))

    def piece_rows(index):
        return pl.ds(pl.multiple_of(index * piece, BLOCK), piece)

    def scatter_copy(m, off):
        return pltpu.make_async_remote_copy(
            src_ref=gsend.at[m, piece_rows(peer(off))],
            dst_ref=rs_recv.at[m, off],
            send_sem=rs_send_sem.at[m, off],
            recv_sem=rs_recv_sem.at[m, off],
            device_id=device_of(peer(off)),
            device_id_type=MESH,
        )

    def gather_copy(m, off):
        return pltpu.make_async_remote_copy(
            src_ref=whole.at[m, piece_rows(chip)],
            dst_ref=whole.at[m, piece_rows(chip)],
            send_sem=ag_send_sem.at[m, off],
            recv_sem=ag_recv_sem.at[m, off],
            device_id=device_of(peer(off)),
            device_id_type=MESH,
        )

    def gather_arrival(m, off):
        source = lax.rem(chip + peers - off, peers)
        return source, pltpu.make_async_remote_copy(
            src_ref=whole.at[m, piece_rows(source)],
            dst_ref=whole.at[m, piece_rows(source)],
            send_sem=ag_send_sem.at[m, off],
            recv_sem=ag_recv_sem.at[m, off],
            device_id=device_of(peer(off)),
            device_id_type=MESH,
        )

    def exchange_copy(g, pos, off):
        there = lax.rem(head + off, head_size)
        start = pl.multiple_of(pos * tokens + there * quarter, BLOCK)
        slot = head * CORES + core
        index = pos * head_size + off
        return pltpu.make_async_remote_copy(
            src_ref=ro_send.at[g, pl.ds(start, quarter)],
            dst_ref=ro_recv.at[g, slot],
            send_sem=ro_send_sem.at[g, index],
            recv_sem=ro_recv_sem.at[g, index],
            device_id=exchange_device(pos, off),
            device_id_type=MESH,
        )

    halves = ((slice(0, tokens), own_ref), (slice(tokens, 2 * tokens), rec_ref))

    def inner_step(g):
        for columns, source in halves:
            keys, signal = source[1, g], source[2, g]
            hid[:, columns] = dot_nt(weights[0], keys)
            gat[:, columns] = dot_nt(weights[1], keys)
            bak[:, columns] = dot_nt(weights[2], signal)

        def pointwise(block, carry):
            at = rows(block)
            hidden, gated, back = hid[at, :], gat[at, :], bak[at, :]
            sigma = jax.nn.sigmoid(hidden)
            act = hidden * sigma
            mixed[at, :] = (act * gated).astype(jnp.bfloat16)
            dgate[at, :] = (back * act).astype(jnp.bfloat16)
            dfirst[at, :] = (back * gated * (sigma * (1.0 + hidden * (1.0 - sigma)))).astype(jnp.bfloat16)
            return carry

        lax.fori_loop(0, hidden_units // BLOCK, pointwise, 0)

        order = ((2, mixed, 2), (1, dgate, 1), (0, dfirst, 1))
        for m, factor, which in order:
            grad = dot(factor[:, :tokens], own_ref[which, g]) + dot(factor[:, tokens:], rec_ref[which, g])
            gsend[m] = grad.astype(jnp.bfloat16)
            for off in range(1, peers):
                guarded(peer(off) < owners, lambda m=m, off=off: scatter_copy(m, off).start())

        for m, _, _ in order:
            def reduce(m=m):
                for off in range(1, peers):
                    scatter_copy(m, off).wait_recv()
                total = gsend[m, piece_rows(chip), :].astype(jnp.float32)
                for off in range(1, peers):
                    total = total + rs_recv[m, off].astype(jnp.float32)
                whole[m, piece_rows(chip), :] = total.astype(jnp.bfloat16)
                for off in range(1, peers):
                    gather_copy(m, off).start()

            guarded(chip < owners, reduce)

        for m, _, _ in order:
            for off in range(1, peers):
                source, arrival = gather_arrival(m, off)
                guarded(source < owners, lambda arrival=arrival: arrival.wait_recv())

            def squares(block, total):
                part = whole[m, rows(block), :].astype(jnp.float32)
                return total + part * part

            total = lax.fori_loop(
                0, hidden_units // BLOCK, squares, jnp.zeros((BLOCK, whole.shape[2]), jnp.float32)
            )
            frob = jnp.sum(jnp.sum(total, axis=0, keepdims=True), axis=1, keepdims=True)
            scale = STEP_SIZE / jnp.sqrt(frob + EPS)

            def refresh(block, carry):
                at = rows(block)
                update = weights[m, at, :].astype(jnp.float32) - scale * whole[m, at, :].astype(jnp.float32)
                length = jnp.sqrt(jnp.sum(update * update, axis=-1, keepdims=True) + EPS)
                weights[m, at, :] = (update * (target[m, at, :] / length)).astype(jnp.bfloat16)
                return carry

            lax.fori_loop(0, hidden_units // BLOCK, refresh, 0)

        for m, _, _ in order:
            for off in range(1, peers):
                guarded(peer(off) < owners, lambda m=m, off=off: scatter_copy(m, off).wait_send())
                guarded(chip < owners, lambda m=m, off=off: gather_copy(m, off).wait_send())

    def group(g, carry):
        def one(_, inner_carry):
            inner_step(g)
            return inner_carry

        lax.fori_loop(0, INNER, one, 0)
        for columns, source in halves:
            queries = source[0, g]
            rhid[columns, :] = dot_nt(queries, weights[0])
            rgat[columns, :] = dot_nt(queries, weights[1])

        def pointwise(block, inner_carry):
            at = rows(block)
            hidden = rhid[at, :]
            rmix[at, :] = (hidden * jax.nn.sigmoid(hidden) * rgat[at, :]).astype(jnp.bfloat16)
            return inner_carry

        lax.fori_loop(0, 2 * tokens // BLOCK, pointwise, 0)
        for columns, _ in halves:
            ro_send[g, columns, :] = dot(rmix[columns, :], weights[2]).astype(jnp.bfloat16)
        for pos, off in exchanges:
            exchange_copy(g, pos, off).start()
        mine = pl.ds(pl.multiple_of(head * quarter, BLOCK), quarter)
        ro_recv[g, head * CORES + core] = ro_send[g, mine, :]
        return carry

    lax.fori_loop(0, groups, group, 0)

    def finish(g, carry):
        for pos, off in exchanges:
            exchange_copy(g, pos, off).wait()
        heads, width = ro_recv.shape[1], ro_recv.shape[3]

        def normalize(block, inner_carry):
            at = rows(block)
            parts = [ro_recv[g, i, at, :].astype(jnp.float32) for i in range(heads)]
            square = sum(jnp.sum(part * part, axis=-1, keepdims=True) for part in parts)
            factor = lax.rsqrt(square / (heads * width) + EPS)
            for i, part in enumerate(parts):
                columns = slice(i * width, (i + 1) * width)
                out_ref[g, at, columns] = (part * factor * gain_ref[:, columns]).astype(jnp.bfloat16)
            return inner_carry

        lax.fori_loop(0, quarter // BLOCK, normalize, 0)
        return carry

    lax.fori_loop(0, groups, finish, 0)


def solution(mesh):
    tok_size, head_size = mesh.shape["tok"], mesh.shape["head"]
    peers = tok_size // CORES

    def body(inputs, projections, lrate, fast_init, gain):
        groups, tokens, _ = inputs.shape
        _, _, units, width = fast_init.shape
        heads = CORES * head_size
        core = lax.axis_index("tok") % CORES
        mapped = jnp.einsum(
            "ctd,sde->scte", inputs, projections, preferred_element_type=jnp.float32
        ).astype(jnp.bfloat16)

        def of_head(which):
            part = lax.dynamic_slice_in_dim(mapped, which * width, width, axis=3)
            rates = lax.dynamic_slice_in_dim(lrate, which, 1, axis=2)
            factor = jnp.concatenate([jnp.ones((2,) + rates.shape, rates.dtype), -rates[None]], axis=0)
            return (part.astype(jnp.float32) * factor).astype(jnp.bfloat16)

        own = of_head(core)
        swap = [(i, i ^ 1) for i in range(tok_size)]
        rec = lax.ppermute(of_head(1 - core), "tok", swap)
        init = lax.dynamic_index_in_dim(fast_init, core, axis=0, keepdims=False)
        piece = -(-units // peers // BLOCK) * BLOCK if units % peers == 0 else BLOCK
        bf16, f32 = jnp.bfloat16, jnp.float32
        return pl.pallas_call(
            functools.partial(train_kernel, tok_size, head_size, piece),
            out_shape=jax.ShapeDtypeStruct((groups, tokens // head_size, heads * width), bf16),
            in_specs=[pl.BlockSpec(memory_space=pltpu.VMEM)] * 4,
            out_specs=pl.BlockSpec(memory_space=pltpu.VMEM),
            scratch_shapes=[
                pltpu.VMEM((3, units, width), bf16),
                pltpu.VMEM((3, units, 1), f32),
                pltpu.VMEM((units, 2 * tokens), f32),
                pltpu.VMEM((units, 2 * tokens), f32),
                pltpu.VMEM((units, 2 * tokens), f32),
                pltpu.VMEM((units, 2 * tokens), bf16),
                pltpu.VMEM((units, 2 * tokens), bf16),
                pltpu.VMEM((units, 2 * tokens), bf16),
                pltpu.VMEM((2 * tokens, units), f32),
                pltpu.VMEM((2 * tokens, units), f32),
                pltpu.VMEM((2 * tokens, units), bf16),
                pltpu.VMEM((3, units, width), bf16),
                pltpu.VMEM((3, peers, piece, width), bf16),
                pltpu.VMEM((3, units, width), bf16),
                pltpu.VMEM((groups, 2 * tokens, width), bf16),
                pltpu.VMEM((groups, heads, tokens // head_size, width), bf16),
                pltpu.SemaphoreType.DMA((3, peers)),
                pltpu.SemaphoreType.DMA((3, peers)),
                pltpu.SemaphoreType.DMA((3, peers)),
                pltpu.SemaphoreType.DMA((3, peers)),
                pltpu.SemaphoreType.DMA((groups, CORES * head_size)),
                pltpu.SemaphoreType.DMA((groups, CORES * head_size)),
            ],
            compiler_params=pltpu.CompilerParams(
                collective_id=0, has_side_effects=True, vmem_limit_bytes=60000 * 1024
            ),
        )(own, rec, init, gain[None])

    return jax.shard_map(
        body,
        mesh=mesh,
        in_specs=(
            P(None, "tok", None),
            P(None, None, "head"),
            P(None, "tok", "head"),
            P("head", None, None, None),
            P(),
        ),
        out_specs=P(None, ("tok", "head"), None),
        check_vma=False,
    )
```

```python
import functools

import jax
import jax.numpy as jnp
from jax import lax
from jax.experimental import pallas as pl
from jax.experimental.pallas import tpu as pltpu
from jax.sharding import PartitionSpec as P

INNER = 2
CORES = 2
STEP_SIZE = 4.0
EPS = 1e-06
MESH = pl.DeviceIdType.MESH
BLOCK = 16
NT = (((1,), (1,)), ((), ()))


def dot(left, right):
    return jnp.dot(left, right, preferred_element_type=jnp.float32)


def dot_nt(left, right):
    return lax.dot_general(left, right, NT, preferred_element_type=jnp.float32)


def train_kernel(
    tok_size, head_size, near_size, piece,
    own_ref, rec_ref, init_ref, gain_ref, out_ref,
    weights, target, hid, gat, bak, mixed, dgate, dfirst, rhid, rgat, rmix,
    gsend, near_recv, partial, far_recv, whole, ro_send, ro_recv,
    sems, ro_send_sem, ro_recv_sem,
):
    groups, tokens = own_ref.shape[1], own_ref.shape[2]
    hidden_units = init_ref.shape[1]
    peers = tok_size // CORES
    far_size = peers // near_size
    owners = hidden_units // near_size // piece
    quarter = tokens // head_size
    tok = lax.axis_index("tok")
    head = lax.axis_index("head")
    chip, core = tok // CORES, tok % CORES
    partner = chip * CORES + (1 - core)

    near, far = chip % near_size, chip // near_size

    def near_peer(offset):
        return lax.rem(near + offset, near_size)

    def far_peer(offset):
        return lax.rem(far + offset, far_size)

    def near_device(offset):
        return {"tok": (far * near_size + near_peer(offset)) * CORES + core, "head": head}

    def far_device(offset):
        return {"tok": (far_peer(offset) * near_size + near) * CORES + core, "head": head}

    def guarded(condition, work):
        if owners == far_size:
            work()
        else:
            pl.when(condition)(work)

    exchanges = [(pos, off) for pos in range(CORES) for off in range(head_size) if (pos, off) != (0, 0)]

    def exchange_device(pos, off):
        return {"tok": tok if pos == 0 else partner, "head": lax.rem(head + off, head_size)}

    barrier = pltpu.get_barrier_semaphore()
    for off in range(1, near_size):
        pl.semaphore_signal(barrier, inc=1, device_id=near_device(off), device_id_type=MESH)
    for off in range(1, far_size):
        pl.semaphore_signal(barrier, inc=1, device_id=far_device(off), device_id_type=MESH)
    for pos, off in exchanges:
        pl.semaphore_signal(barrier, inc=1, device_id=exchange_device(pos, off), device_id_type=MESH)

    def rows(block):
        return pl.ds(pl.multiple_of(block * BLOCK, BLOCK), BLOCK)

    for m in range(3):
        def prepare(block, carry, m=m):
            start = init_ref[m, rows(block), :]
            weights[m, rows(block), :] = start
            start = start.astype(jnp.float32)
            target[m, rows(block), :] = jnp.sqrt(jnp.sum(start * start, axis=-1, keepdims=True))
            return carry

        lax.fori_loop(0, hidden_units // BLOCK, prepare, 0)

    pl.semaphore_wait(barrier, near_size - 1 + far_size - 1 + len(exchanges))

    span = hidden_units // near_size

    def span_rows(index):
        return pl.ds(pl.multiple_of(index * span, BLOCK), span)

    def piece_rows(index, base=0):
        return pl.ds(pl.multiple_of(base + index * piece, BLOCK), piece)

    def remote(source, target, sems, m, off, device):
        return pltpu.make_async_remote_copy(
            src_ref=source,
            dst_ref=target,
            send_sem=sems[0].at[m, off],
            recv_sem=sems[1].at[m, off],
            device_id=device,
            device_id_type=MESH,
        )

    def near_scatter(m, off):
        index = near_peer(off)
        return remote(
            gsend.at[m, span_rows(index)], near_recv.at[m, off], (sems.at[0], sems.at[1]), m, off, near_device(off)
        )

    def far_scatter(m, off):
        return remote(
            partial.at[m, piece_rows(far_peer(off))], far_recv.at[m, off], (sems.at[2], sems.at[3]), m, off, far_device(off)
        )

    def far_gather(m, off, source=far):
        at = piece_rows(source, near * span)
        return remote(whole.at[m, at], whole.at[m, at], (sems.at[4], sems.at[5]), m, off, far_device(off))

    def near_gather(m, off, source=near):
        at = span_rows(source)
        return remote(whole.at[m, at], whole.at[m, at], (sems.at[6], sems.at[7]), m, off, near_device(off))

    def exchange_copy(g, pos, off):
        there = lax.rem(head + off, head_size)
        start = pl.multiple_of(pos * tokens + there * quarter, BLOCK)
        slot = head * CORES + core
        index = pos * head_size + off
        return pltpu.make_async_remote_copy(
            src_ref=ro_send.at[g, pl.ds(start, quarter)],
            dst_ref=ro_recv.at[g, slot],
            send_sem=ro_send_sem.at[g, index],
            recv_sem=ro_recv_sem.at[g, index],
            device_id=exchange_device(pos, off),
            device_id_type=MESH,
        )

    halves = ((slice(0, tokens), own_ref), (slice(tokens, 2 * tokens), rec_ref))

    def inner_step(g):
        for columns, source in halves:
            keys, signal = source[1, g], source[2, g]
            hid[:, columns] = dot_nt(weights[0], keys)
            gat[:, columns] = dot_nt(weights[1], keys)
            bak[:, columns] = dot_nt(weights[2], signal)

        def pointwise(block, carry):
            at = rows(block)
            hidden, gated, back = hid[at, :], gat[at, :], bak[at, :]
            sigma = jax.nn.sigmoid(hidden)
            act = hidden * sigma
            mixed[at, :] = (act * gated).astype(jnp.bfloat16)
            dgate[at, :] = (back * act).astype(jnp.bfloat16)
            dfirst[at, :] = (back * gated * (sigma * (1.0 + hidden * (1.0 - sigma)))).astype(jnp.bfloat16)
            return carry

        lax.fori_loop(0, hidden_units // BLOCK, pointwise, 0)

        order = ((2, mixed, 2), (1, dgate, 1), (0, dfirst, 1))
        for m, factor, which in order:
            grad = dot(factor[:, :tokens], own_ref[which, g]) + dot(factor[:, tokens:], rec_ref[which, g])
            gsend[m] = grad.astype(jnp.bfloat16)
            for off in range(1, near_size):
                near_scatter(m, off).start()

        def reduce_near(m):
            for off in range(1, near_size):
                near_scatter(m, off).wait_recv()
            total = gsend[m, span_rows(near), :].astype(jnp.float32)
            for off in range(1, near_size):
                total = total + near_recv[m, off].astype(jnp.float32)
            partial[m] = total.astype(jnp.bfloat16)
            for off in range(1, far_size):
                guarded(far_peer(off) < owners, lambda off=off: far_scatter(m, off).start())

        def reduce_far(m):
            def work():
                for off in range(1, far_size):
                    far_scatter(m, off).wait_recv()
                total = partial[m, piece_rows(far), :].astype(jnp.float32)
                for off in range(1, far_size):
                    total = total + far_recv[m, off].astype(jnp.float32)
                whole[m, piece_rows(far, near * span), :] = total.astype(jnp.bfloat16)
                for off in range(1, far_size):
                    far_gather(m, off).start()

            guarded(far < owners, work)

        def spread(m):
            for off in range(1, far_size):
                source = lax.rem(far + far_size - off, far_size)
                guarded(source < owners, lambda off=off, source=source: far_gather(m, off, source).wait_recv())
            for off in range(1, near_size):
                near_gather(m, off).start()

        def update_memory(m):
            for off in range(1, near_size):
                near_gather(m, off, lax.rem(near + near_size - off, near_size)).wait_recv()

            def squares(block, total):
                part = whole[m, rows(block), :].astype(jnp.float32)
                return total + part * part

            total = lax.fori_loop(
                0, hidden_units // BLOCK, squares, jnp.zeros((BLOCK, whole.shape[2]), jnp.float32)
            )
            frob = jnp.sum(jnp.sum(total, axis=0, keepdims=True), axis=1, keepdims=True)
            scale = STEP_SIZE / jnp.sqrt(frob + EPS)

            def refresh(block, carry):
                at = rows(block)
                update = weights[m, at, :].astype(jnp.float32) - scale * whole[m, at, :].astype(jnp.float32)
                length = jnp.sqrt(jnp.sum(update * update, axis=-1, keepdims=True) + EPS)
                weights[m, at, :] = (update * (target[m, at, :] / length)).astype(jnp.bfloat16)
                return carry

            lax.fori_loop(0, hidden_units // BLOCK, refresh, 0)

        stages = (reduce_near, reduce_far, spread, update_memory)
        for turn in range(len(order) + len(stages) - 1):
            for depth, stage in enumerate(stages):
                if 0 <= turn - depth < len(order):
                    stage(order[turn - depth][0])

        for m, _, _ in order:
            for off in range(1, near_size):
                near_scatter(m, off).wait_send()
                near_gather(m, off).wait_send()
            for off in range(1, far_size):
                guarded(far_peer(off) < owners, lambda m=m, off=off: far_scatter(m, off).wait_send())
                guarded(far < owners, lambda m=m, off=off: far_gather(m, off).wait_send())

    def group(g, carry):
        def one(_, inner_carry):
            inner_step(g)
            return inner_carry

        lax.fori_loop(0, INNER, one, 0)
        for columns, source in halves:
            queries = source[0, g]
            rhid[columns, :] = dot_nt(queries, weights[0])
            rgat[columns, :] = dot_nt(queries, weights[1])

        def pointwise(block, inner_carry):
            at = rows(block)
            hidden = rhid[at, :]
            rmix[at, :] = (hidden * jax.nn.sigmoid(hidden) * rgat[at, :]).astype(jnp.bfloat16)
            return inner_carry

        lax.fori_loop(0, 2 * tokens // BLOCK, pointwise, 0)
        for columns, _ in halves:
            ro_send[g, columns, :] = dot(rmix[columns, :], weights[2]).astype(jnp.bfloat16)
        for pos, off in exchanges:
            exchange_copy(g, pos, off).start()
        mine = pl.ds(pl.multiple_of(head * quarter, BLOCK), quarter)
        ro_recv[g, head * CORES + core] = ro_send[g, mine, :]
        return carry

    lax.fori_loop(0, groups, group, 0)

    def finish(g, carry):
        for pos, off in exchanges:
            exchange_copy(g, pos, off).wait()
        heads, width = ro_recv.shape[1], ro_recv.shape[3]

        def normalize(block, inner_carry):
            at = rows(block)
            parts = [ro_recv[g, i, at, :].astype(jnp.float32) for i in range(heads)]
            square = sum(jnp.sum(part * part, axis=-1, keepdims=True) for part in parts)
            factor = lax.rsqrt(square / (heads * width) + EPS)
            for i, part in enumerate(parts):
                columns = slice(i * width, (i + 1) * width)
                out_ref[g, at, columns] = (part * factor * gain_ref[:, columns]).astype(jnp.bfloat16)
            return inner_carry

        lax.fori_loop(0, quarter // BLOCK, normalize, 0)
        return carry

    lax.fori_loop(0, groups, finish, 0)


def solution(mesh):
    tok_size, head_size = mesh.shape["tok"], mesh.shape["head"]
    peers = tok_size // CORES

    def body(inputs, projections, lrate, fast_init, gain):
        groups, tokens, _ = inputs.shape
        _, _, units, width = fast_init.shape
        heads = CORES * head_size
        core = lax.axis_index("tok") % CORES
        mapped = jnp.einsum(
            "ctd,sde->scte", inputs, projections, preferred_element_type=jnp.float32
        ).astype(jnp.bfloat16)

        def of_head(which):
            part = lax.dynamic_slice_in_dim(mapped, which * width, width, axis=3)
            rates = lax.dynamic_slice_in_dim(lrate, which, 1, axis=2)
            factor = jnp.concatenate([jnp.ones((2,) + rates.shape, rates.dtype), -rates[None]], axis=0)
            return (part.astype(jnp.float32) * factor).astype(jnp.bfloat16)

        own = of_head(core)
        swap = [(i, i ^ 1) for i in range(tok_size)]
        rec = lax.ppermute(of_head(1 - core), "tok", swap)
        init = lax.dynamic_index_in_dim(fast_init, core, axis=0, keepdims=False)
        near_size = min(4, peers)
        far_size = peers // near_size
        span = units // near_size
        piece = span // far_size if span % (far_size * BLOCK) == 0 else BLOCK
        bf16, f32 = jnp.bfloat16, jnp.float32
        return pl.pallas_call(
            functools.partial(train_kernel, tok_size, head_size, near_size, piece),
            out_shape=jax.ShapeDtypeStruct((groups, tokens // head_size, heads * width), bf16),
            in_specs=[pl.BlockSpec(memory_space=pltpu.VMEM)] * 4,
            out_specs=pl.BlockSpec(memory_space=pltpu.VMEM),
            scratch_shapes=[
                pltpu.VMEM((3, units, width), bf16),
                pltpu.VMEM((3, units, 1), f32),
                pltpu.VMEM((units, 2 * tokens), f32),
                pltpu.VMEM((units, 2 * tokens), f32),
                pltpu.VMEM((units, 2 * tokens), f32),
                pltpu.VMEM((units, 2 * tokens), bf16),
                pltpu.VMEM((units, 2 * tokens), bf16),
                pltpu.VMEM((units, 2 * tokens), bf16),
                pltpu.VMEM((2 * tokens, units), f32),
                pltpu.VMEM((2 * tokens, units), f32),
                pltpu.VMEM((2 * tokens, units), bf16),
                pltpu.VMEM((3, units, width), bf16),
                pltpu.VMEM((3, near_size, span, width), bf16),
                pltpu.VMEM((3, span, width), bf16),
                pltpu.VMEM((3, far_size, piece, width), bf16),
                pltpu.VMEM((3, units, width), bf16),
                pltpu.VMEM((groups, 2 * tokens, width), bf16),
                pltpu.VMEM((groups, heads, tokens // head_size, width), bf16),
                pltpu.SemaphoreType.DMA((8, 3, max(near_size, far_size))),
                pltpu.SemaphoreType.DMA((groups, CORES * head_size)),
                pltpu.SemaphoreType.DMA((groups, CORES * head_size)),
            ],
            compiler_params=pltpu.CompilerParams(
                collective_id=0, has_side_effects=True, vmem_limit_bytes=60000 * 1024
            ),
        )(own, rec, init, gain[None])

    return jax.shard_map(
        body,
        mesh=mesh,
        in_specs=(
            P(None, "tok", None),
            P(None, None, "head"),
            P(None, "tok", "head"),
            P("head", None, None, None),
            P(),
        ),
        out_specs=P(None, ("tok", "head"), None),
        check_vma=False,
    )
```

```python
import functools

import jax
import jax.numpy as jnp
from jax import lax
from jax.experimental import pallas as pl
from jax.experimental.pallas import tpu as pltpu
from jax.sharding import PartitionSpec as P

INNER = 2
CORES = 2
STEP_SIZE = 4.0
EPS = 1e-06
MESH = pl.DeviceIdType.MESH
BLOCK = 16
NT = (((1,), (1,)), ((), ()))


def dot(left, right):
    return jnp.dot(left, right, preferred_element_type=jnp.float32)


def dot_nt(left, right):
    return lax.dot_general(left, right, NT, preferred_element_type=jnp.float32)


class Chunk:
    def __init__(self, m, base, near_size, peers, chip, part):
        self.m, self.base, self.near_size = m, base, near_size
        self.far_size = peers // near_size
        self.near, self.far = chip % near_size, chip // near_size
        self.span = part // near_size
        self.piece = piece_of(part, near_size, peers)
        self.owners = self.span // self.piece

    def near_peer(self, off):
        return lax.rem(self.near + off, self.near_size)

    def far_peer(self, off):
        return lax.rem(self.far + off, self.far_size)

    def near_chip(self, off):
        return self.far * self.near_size + self.near_peer(off)

    def far_chip(self, off):
        return self.far_peer(off) * self.near_size + self.near

    def span_rows(self, index):
        return pl.ds(pl.multiple_of(self.base + index * self.span, BLOCK), self.span)

    def piece_rows(self, index):
        return pl.ds(pl.multiple_of(self.base + self.near * self.span + index * self.piece, BLOCK), self.piece)

    def guarded(self, index, work):
        if self.owners == self.far_size:
            work()
        else:
            pl.when(index < self.owners)(work)


def piece_of(part, near_size, peers):
    span, far_size = part // near_size, peers // near_size
    return span // far_size if span % (far_size * BLOCK) == 0 else BLOCK


def train_kernel(
    tok_size, head_size, near_sizes, part,
    own_ref, rec_ref, init_ref, gain_ref, out_ref,
    weights, target, hid, gat, bak, mixed, dgate, dfirst, rhid, rgat, rmix,
    gsend, near_recv, partial, far_recv, whole, ro_send, ro_recv,
    sems, ro_send_sem, ro_recv_sem,
):
    groups, tokens = own_ref.shape[1], own_ref.shape[2]
    hidden_units = init_ref.shape[1]
    peers = tok_size // CORES
    quarter = tokens // head_size
    tok = lax.axis_index("tok")
    head = lax.axis_index("head")
    chip, core = tok // CORES, tok % CORES
    partner = chip * CORES + (1 - core)


    def chip_device(index):
        return {"tok": index * CORES + core, "head": head}

    chunks = [
        Chunk(m, base, near_sizes[i % len(near_sizes)], peers, chip, part)
        for i, (base, m) in enumerate((base, m) for base in range(0, hidden_units, part) for m in (2, 1, 0))
    ]

    exchanges = [(pos, off) for pos in range(CORES) for off in range(head_size) if (pos, off) != (0, 0)]

    def exchange_device(pos, off):
        return {"tok": tok if pos == 0 else partner, "head": lax.rem(head + off, head_size)}

    barrier = pltpu.get_barrier_semaphore()
    for off in range(1, peers):
        pl.semaphore_signal(barrier, inc=1, device_id=chip_device(lax.rem(chip + off, peers)), device_id_type=MESH)
    for pos, off in exchanges:
        pl.semaphore_signal(barrier, inc=1, device_id=exchange_device(pos, off), device_id_type=MESH)

    def rows(block):
        return pl.ds(pl.multiple_of(block * BLOCK, BLOCK), BLOCK)

    for m in range(3):
        def prepare(block, carry, m=m):
            start = init_ref[m, rows(block), :]
            weights[m, rows(block), :] = start
            start = start.astype(jnp.float32)
            target[m, rows(block), :] = jnp.sqrt(jnp.sum(start * start, axis=-1, keepdims=True))
            return carry

        lax.fori_loop(0, hidden_units // BLOCK, prepare, 0)

    pl.semaphore_wait(barrier, peers - 1 + len(exchanges))

    def remote(source, target, kind, c, off, device):
        return pltpu.make_async_remote_copy(
            src_ref=source,
            dst_ref=target,
            send_sem=sems.at[kind, c, off],
            recv_sem=sems.at[kind + 1, c, off],
            device_id=device,
            device_id_type=MESH,
        )

    def near_scatter(c, off):
        k = chunks[c]
        slot = near_recv.at[c, off, pl.ds(0, k.span)]
        return remote(gsend.at[k.m, k.span_rows(k.near_peer(off))], slot, 0, c, off, chip_device(k.near_chip(off)))

    def far_scatter(c, off):
        k = chunks[c]
        source = partial.at[c, pl.ds(pl.multiple_of(k.far_peer(off) * k.piece, BLOCK), k.piece)]
        return remote(source, far_recv.at[c, off, pl.ds(0, k.piece)], 2, c, off, chip_device(k.far_chip(off)))

    def far_gather(c, off, source=None):
        k = chunks[c]
        at = k.piece_rows(k.far if source is None else source)
        return remote(whole.at[k.m, at], whole.at[k.m, at], 4, c, off, chip_device(k.far_chip(off)))

    def near_gather(c, off, source=None):
        k = chunks[c]
        at = k.span_rows(k.near if source is None else source)
        return remote(whole.at[k.m, at], whole.at[k.m, at], 6, c, off, chip_device(k.near_chip(off)))

    def exchange_copy(g, pos, off):
        there = lax.rem(head + off, head_size)
        start = pl.multiple_of(pos * tokens + there * quarter, BLOCK)
        slot = head * CORES + core
        index = pos * head_size + off
        return pltpu.make_async_remote_copy(
            src_ref=ro_send.at[g, pl.ds(start, quarter)],
            dst_ref=ro_recv.at[g, slot],
            send_sem=ro_send_sem.at[g, index],
            recv_sem=ro_recv_sem.at[g, index],
            device_id=exchange_device(pos, off),
            device_id_type=MESH,
        )

    halves = ((slice(0, tokens), own_ref), (slice(tokens, 2 * tokens), rec_ref))

    def inner_step(g):
        def compute(base):
            units = pl.ds(base, part)
            for columns, source in halves:
                keys, signal = source[1, g], source[2, g]
                hid[:, columns] = dot_nt(weights[0, units, :], keys)
                gat[:, columns] = dot_nt(weights[1, units, :], keys)
                bak[:, columns] = dot_nt(weights[2, units, :], signal)

            def pointwise(block, carry):
                at = rows(block)
                hidden, gated, back = hid[at, :], gat[at, :], bak[at, :]
                sigma = jax.nn.sigmoid(hidden)
                act = hidden * sigma
                mixed[at, :] = (act * gated).astype(jnp.bfloat16)
                dgate[at, :] = (back * act).astype(jnp.bfloat16)
                dfirst[at, :] = (back * gated * (sigma * (1.0 + hidden * (1.0 - sigma)))).astype(jnp.bfloat16)
                return carry

            lax.fori_loop(0, part // BLOCK, pointwise, 0)
            for m, factor, which in ((2, mixed, 2), (1, dgate, 1), (0, dfirst, 1)):
                grad = dot(factor[:, :tokens], own_ref[which, g]) + dot(factor[:, tokens:], rec_ref[which, g])
                gsend[m, units, :] = grad.astype(jnp.bfloat16)
                for c, k in enumerate(chunks):
                    if (k.m, k.base) == (m, base):
                        for off in range(1, k.near_size):
                            near_scatter(c, off).start()

        def reduce_near(c):
            k = chunks[c]
            for off in range(1, k.near_size):
                near_scatter(c, off).wait_recv()
            total = gsend[k.m, k.span_rows(k.near), :].astype(jnp.float32)
            for off in range(1, k.near_size):
                total = total + near_recv[c, off, : k.span].astype(jnp.float32)
            partial[c, : k.span] = total.astype(jnp.bfloat16)
            for off in range(1, k.far_size):
                k.guarded(k.far_peer(off), lambda off=off: far_scatter(c, off).start())

        def reduce_far(c):
            k = chunks[c]

            def work():
                for off in range(1, k.far_size):
                    far_scatter(c, off).wait_recv()
                mine = pl.ds(pl.multiple_of(k.far * k.piece, BLOCK), k.piece)
                total = partial[c, mine, :].astype(jnp.float32)
                for off in range(1, k.far_size):
                    total = total + far_recv[c, off, : k.piece].astype(jnp.float32)
                whole[k.m, k.piece_rows(k.far), :] = total.astype(jnp.bfloat16)
                for off in range(1, k.far_size):
                    far_gather(c, off).start()

            k.guarded(k.far, work)

        def spread(c):
            k = chunks[c]
            for off in range(1, k.far_size):
                source = k.far_peer(k.far_size - off)
                k.guarded(source, lambda off=off, source=source: far_gather(c, off, source).wait_recv())
            for off in range(1, k.near_size):
                near_gather(c, off).start()

        def collect(c):
            k = chunks[c]
            for off in range(1, k.near_size):
                near_gather(c, off, k.near_peer(k.near_size - off)).wait_recv()
            if k.base + part == hidden_units:
                update_memory(k.m)

        def update_memory(m):
            def squares(block, total):
                part = whole[m, rows(block), :].astype(jnp.float32)
                return total + part * part

            total = lax.fori_loop(
                0, hidden_units // BLOCK, squares, jnp.zeros((BLOCK, whole.shape[2]), jnp.float32)
            )
            frob = jnp.sum(jnp.sum(total, axis=0, keepdims=True), axis=1, keepdims=True)
            scale = STEP_SIZE / jnp.sqrt(frob + EPS)

            def refresh(block, carry):
                at = rows(block)
                update = weights[m, at, :].astype(jnp.float32) - scale * whole[m, at, :].astype(jnp.float32)
                length = jnp.sqrt(jnp.sum(update * update, axis=-1, keepdims=True) + EPS)
                weights[m, at, :] = (update * (target[m, at, :] / length)).astype(jnp.bfloat16)
                return carry

            lax.fori_loop(0, hidden_units // BLOCK, refresh, 0)

        stages = (reduce_near, reduce_far, spread, collect)
        bases = list(range(0, hidden_units, part))
        for base in bases[:2]:
            compute(base)
        for turn in range(len(chunks) + len(stages) - 1):
            for depth, stage in enumerate(stages):
                if 0 <= turn - depth < len(chunks):
                    stage(turn - depth)
            if turn % 3 == 1 and turn // 3 + 2 < len(bases):
                compute(bases[turn // 3 + 2])

        for c, k in enumerate(chunks):
            for off in range(1, k.near_size):
                near_scatter(c, off).wait_send()
                near_gather(c, off).wait_send()
            for off in range(1, k.far_size):
                k.guarded(k.far_peer(off), lambda c=c, off=off: far_scatter(c, off).wait_send())
                k.guarded(k.far, lambda c=c, off=off: far_gather(c, off).wait_send())

    def group(g, carry):
        def one(_, inner_carry):
            inner_step(g)
            return inner_carry

        lax.fori_loop(0, INNER, one, 0)
        for columns, source in halves:
            queries = source[0, g]
            rhid[columns, :] = dot_nt(queries, weights[0])
            rgat[columns, :] = dot_nt(queries, weights[1])

        def pointwise(block, inner_carry):
            at = rows(block)
            hidden = rhid[at, :]
            rmix[at, :] = (hidden * jax.nn.sigmoid(hidden) * rgat[at, :]).astype(jnp.bfloat16)
            return inner_carry

        lax.fori_loop(0, 2 * tokens // BLOCK, pointwise, 0)
        for columns, _ in halves:
            ro_send[g, columns, :] = dot(rmix[columns, :], weights[2]).astype(jnp.bfloat16)
        for pos, off in exchanges:
            exchange_copy(g, pos, off).start()
        mine = pl.ds(pl.multiple_of(head * quarter, BLOCK), quarter)
        ro_recv[g, head * CORES + core] = ro_send[g, mine, :]
        return carry

    lax.fori_loop(0, groups, group, 0)

    def finish(g, carry):
        for pos, off in exchanges:
            exchange_copy(g, pos, off).wait()
        heads, width = ro_recv.shape[1], ro_recv.shape[3]

        def normalize(block, inner_carry):
            at = rows(block)
            parts = [ro_recv[g, i, at, :].astype(jnp.float32) for i in range(heads)]
            square = sum(jnp.sum(part * part, axis=-1, keepdims=True) for part in parts)
            factor = lax.rsqrt(square / (heads * width) + EPS)
            for i, part in enumerate(parts):
                columns = slice(i * width, (i + 1) * width)
                out_ref[g, at, columns] = (part * factor * gain_ref[:, columns]).astype(jnp.bfloat16)
            return inner_carry

        lax.fori_loop(0, quarter // BLOCK, normalize, 0)
        return carry

    lax.fori_loop(0, groups, finish, 0)


def solution(mesh):
    tok_size, head_size = mesh.shape["tok"], mesh.shape["head"]
    peers = tok_size // CORES

    def body(inputs, projections, lrate, fast_init, gain):
        groups, tokens, _ = inputs.shape
        _, _, units, width = fast_init.shape
        heads = CORES * head_size
        core = lax.axis_index("tok") % CORES
        mapped = jnp.einsum(
            "ctd,sde->scte", inputs, projections, preferred_element_type=jnp.float32
        ).astype(jnp.bfloat16)

        def of_head(which):
            part = lax.dynamic_slice_in_dim(mapped, which * width, width, axis=3)
            rates = lax.dynamic_slice_in_dim(lrate, which, 1, axis=2)
            factor = jnp.concatenate([jnp.ones((2,) + rates.shape, rates.dtype), -rates[None]], axis=0)
            return (part.astype(jnp.float32) * factor).astype(jnp.bfloat16)

        own = of_head(core)
        swap = [(i, i ^ 1) for i in range(tok_size)]
        rec = lax.ppermute(of_head(1 - core), "tok", swap)
        init = lax.dynamic_index_in_dim(fast_init, core, axis=0, keepdims=False)
        near_sizes = (4, 2) if peers <= 8 else (4,)
        part = units // 3 if units % 3 == 0 and units // 3 % (4 * BLOCK) == 0 else units
        count = 3 * (units // part)
        span = max(part // size for size in near_sizes)
        near_most = max(near_sizes)
        far_most = max(peers // size for size in near_sizes)
        piece = max(piece_of(part, size, peers) for size in near_sizes)
        bf16, f32 = jnp.bfloat16, jnp.float32
        return pl.pallas_call(
            functools.partial(train_kernel, tok_size, head_size, near_sizes, part),
            out_shape=jax.ShapeDtypeStruct((groups, tokens // head_size, heads * width), bf16),
            in_specs=[pl.BlockSpec(memory_space=pltpu.VMEM)] * 4,
            out_specs=pl.BlockSpec(memory_space=pltpu.VMEM),
            scratch_shapes=[
                pltpu.VMEM((3, units, width), bf16),
                pltpu.VMEM((3, units, 1), f32),
                pltpu.VMEM((part, 2 * tokens), f32),
                pltpu.VMEM((part, 2 * tokens), f32),
                pltpu.VMEM((part, 2 * tokens), f32),
                pltpu.VMEM((part, 2 * tokens), bf16),
                pltpu.VMEM((part, 2 * tokens), bf16),
                pltpu.VMEM((part, 2 * tokens), bf16),
                pltpu.VMEM((2 * tokens, units), f32),
                pltpu.VMEM((2 * tokens, units), f32),
                pltpu.VMEM((2 * tokens, units), bf16),
                pltpu.VMEM((3, units, width), bf16),
                pltpu.VMEM((count, near_most, span, width), bf16),
                pltpu.VMEM((count, span, width), bf16),
                pltpu.VMEM((count, far_most, piece, width), bf16),
                pltpu.VMEM((3, units, width), bf16),
                pltpu.VMEM((groups, 2 * tokens, width), bf16),
                pltpu.VMEM((groups, heads, tokens // head_size, width), bf16),
                pltpu.SemaphoreType.DMA((8, count, max(near_most, far_most))),
                pltpu.SemaphoreType.DMA((groups, CORES * head_size)),
                pltpu.SemaphoreType.DMA((groups, CORES * head_size)),
            ],
            compiler_params=pltpu.CompilerParams(
                collective_id=0, has_side_effects=True, vmem_limit_bytes=60000 * 1024
            ),
        )(own, rec, init, gain[None])

    return jax.shard_map(
        body,
        mesh=mesh,
        in_specs=(
            P(None, "tok", None),
            P(None, None, "head"),
            P(None, "tok", "head"),
            P("head", None, None, None),
            P(),
        ),
        out_specs=P(None, ("tok", "head"), None),
        check_vma=False,
    )
```
